32 devices in a mesh: gz: 8 (over z, x), gy: 4 (over y, core).
Axes of the slice: x: 2, y: 2, z: 4, core: 2. Of those that a mesh axis runs over, the one named last changes fastest.
Arguments:
- source: float32 [32, 64, 512], P('gz', 'gy'), may hold values from -8 to 8
- conduct: float32 [32, 64, 512], P('gz', 'gy'), may hold values from 0.5 to 4
Outputs:
- adjoint: float32 [32, 64, 512], P('gz', 'gy')
- residual: float32 [32, 64, 512], P('gz', 'gy')
The draws below stay inside these ranges and needn't reach their ends.
All inputs are finite; a program needn't handle non-finite values.
Results may differ from the reference program's by a relative error of at most 0.0003.
Values sent between devices are 32-bit elements; how exact they have to be, the bound alone decides.
A program may use at most 64 MiB of HBM per device.

```python
import math
import jax
import jax.numpy as jnp

NX = 512
DEGREE = 3
COARSE_DEGREE = 4
CYCLES = 2
NZ = 32
NY = 64


def levels(stream_key, dims, split, least, largest):
    gain, own = 1.0, jax.random.fold_in(stream_key, 6)
    for axis_at, shards_of in split:
        heights = jnp.exp(jax.random.uniform(jax.random.fold_in(own, axis_at), (shards_of,), jnp.float32, least / len(split), largest / len(split)))
        gain = gain * jnp.repeat(heights, dims[axis_at] // shards_of).reshape([-1 if axis == axis_at else 1 for axis in range(len(dims))])
    return gain


def normal_values(stream_key, extent, deviation, most, cuts=(), kind=jnp.bfloat16):
    factor_of = levels(stream_key, extent, cuts, -0.22, 0.18) if cuts else 1.0
    entries = jax.random.normal(stream_key, extent, jnp.float32) * deviation * factor_of
    return jnp.minimum(jnp.maximum(entries, -most), most).astype(kind)


def setup_inputs(seed: int = 0) -> dict:
    splits = jax.random.split(jax.random.key(seed), 3)
    source = normal_values(splits[0], (NZ, NY, NX), 1.0, 8.0, ((0, 8), (1, 4)), jnp.float32)
    conduct = jnp.clip(jnp.exp(math.log(4.0) - 2.0794415 * jax.random.uniform(splits[1], (NZ, NY, NX), jnp.float32) ** levels(splits[1], (NZ, NY, NX), ((0, 8), (1, 4)), -0.2, 0.2)), 0.5, 4.0)
    return {"source": source, "conduct": conduct}


cheb_low = 0.3
cheb_high = 1.9
heat_step = 4.0


def apply_level(field, conduct, scale):
    w = conduct * field
    beside = jnp.roll(w, -1, 0) + jnp.roll(w, 1, 0)
    beside = beside + jnp.roll(w, -1, 1) + jnp.roll(w, 1, 1)
    padded = jnp.pad(w, ((0, 0), (0, 0), (1, 1)))
    beside = beside + padded[:, :, 2:] + padded[:, :, :-2]
    return field + scale * (6.0 * w - beside)


def restrict(field):
    z, y, x = field.shape
    return field.reshape(z // 2, 2, y // 2, 2, x // 2, 2).mean(axis=(1, 3, 5))


def prolong(field):
    return jnp.repeat(jnp.repeat(jnp.repeat(field, 2, 0), 2, 1), 2, 2)


def smooth(apply_fn, rhs, start, inv_diag, steps):
    theta = (cheb_high + cheb_low) / 2.0
    delta = (cheb_high - cheb_low) / 2.0
    sigma = theta / delta
    rho = 1.0 / sigma
    if start is None:
        correct = inv_diag * rhs
        change = correct / theta
        field = change
    else:
        correct = inv_diag * (rhs - apply_fn(start))
        change = correct / theta
        field = start + change
    for step in range(steps - 1):
        rho_next = 1.0 / (2.0 * sigma - rho)
        correct = inv_diag * (rhs - apply_fn(field))
        change = rho_next * rho * change + (2.0 * rho_next / delta) * correct
        field = field + change
        rho = rho_next
    return field


def vcycle(rhs, conducts, scales):
    ops = [partial_apply(conducts[i], scales[i]) for i in range(3)]
    diags = [1.0 / (1.0 + 6.0 * scales[i] * conducts[i]) for i in range(3)]
    fine = smooth(ops[0], rhs, None, diags[0], DEGREE)
    rhs_mid = restrict(rhs - ops[0](fine))
    middle = smooth(ops[1], rhs_mid, None, diags[1], DEGREE)
    rhs_low = restrict(rhs_mid - ops[1](middle))
    lowest = smooth(ops[2], rhs_low, None, diags[2], COARSE_DEGREE)
    middle = smooth(ops[1], rhs_mid, middle + prolong(lowest), diags[1], DEGREE)
    fine = smooth(ops[0], rhs, fine + prolong(middle), diags[0], DEGREE)
    return fine


def partial_apply(conduct, scale):
    def inner(field):
        return apply_level(field, conduct, scale)
    return inner


def reference(source, conduct):
    mid_cond = restrict(conduct)
    conducts = [conduct, mid_cond, restrict(mid_cond)]
    scales = [heat_step, heat_step / 4.0, heat_step / 16.0]
    adjoint = jnp.zeros_like(source)
    remain = source
    for cycle in range(CYCLES):
        adjoint = adjoint + vcycle(remain, conducts, scales)
        remain = source - apply_level(adjoint, conduct, heat_step)
    return adjoint, remain
```

```python
import functools

import jax
import jax.numpy as jnp
from jax import lax
from jax.experimental import pallas as pl
from jax.experimental.pallas import tpu as pltpu
from jax.sharding import PartitionSpec as P

DEGREE = 3
COARSE_DEGREE = 4

cheb_low = 0.3
cheb_high = 1.9
heat_step = 4.0

HALO = 4
PAD = 8
EDGE = 16
MID_REACH = 15
MESH = pl.DeviceIdType.MESH
LANES = 128
TILE = 8


def coefficients(steps):
    theta = (cheb_high + cheb_low) / 2.0
    delta = (cheb_high - cheb_low) / 2.0
    sigma = theta / delta
    rho = 1.0 / sigma
    pairs = [(0.0, 1.0 / theta)]
    for _ in range(steps - 1):
        rho_next = 1.0 / (2.0 * sigma - rho)
        pairs.append((rho_next * rho, 2.0 * rho_next / delta))
        rho = rho_next
    return pairs


def window(devices, reach):
    count = min(2 * reach + 1, devices)
    ahead = count // 2
    return [s if s <= ahead else s - count for s in range(count)]


def parts_of(value, count):
    parts = []
    for _ in range(count):
        parts.append(value.astype(jnp.bfloat16))
        value = value - parts[-1].astype(jnp.float32)
    return parts


def pick_columns(value, columns, count):
    total = None
    for part in reversed(parts_of(value, count)):
        term = jnp.dot(part, columns, preferred_element_type=jnp.float32)
        total = term if total is None else total + term
    return total


def unrolled(count, most):
    return max(u for u in range(1, most + 1) if count % u == 0)


def loop(count, body, most=2):
    def step(i, carry):
        body(i)
        return carry

    lax.fori_loop(0, count, step, 0, unroll=unrolled(count, most))


def rows_at(ref, p, c, row):
    return ref[p, c, pl.ds(row, TILE)]


def beside_of(w, p, row):
    planes, chunks = w.shape[0], w.shape[1]
    after, before = lax.rem(p + 1, planes), lax.rem(p + planes - 1, planes)
    here = [rows_at(w, p, c, row) for c in range(chunks)]
    lane = lax.broadcasted_iota(jnp.int32, here[0].shape, 1)
    first = jnp.where(lane == 0, 0.0, pltpu.roll(here[-1], 1, 1))
    last = jnp.where(lane == LANES - 1, 0.0, pltpu.roll(here[0], LANES - 1, 1))
    around = [first] + here + [last]
    beside = []
    for c in range(chunks):
        total = rows_at(w, after, c, row) + rows_at(w, before, c, row)
        total = total + (rows_at(w, p, c, row - 1) + rows_at(w, p, c, row + 1))
        beside.append(total + (around[c] + around[c + 2]))
    return here, beside


class Level:
    def __init__(self, k, m, g, inverse, d, wa, wb, rows, wraps, most):
        self.k, self.m, self.g, self.inverse, self.d = k, m, g, inverse, d
        self.w = (wa, wb)
        self.rows, self.wraps, self.most = rows, wraps, most

    def run(self, planes, body):
        first, count = planes

        def at(i):
            body(lax.rem(i + first, self.k.shape[0]))

        loop(count, at, self.most)

    def put(self, ref, p, c, row, value):
        ref[p, c, pl.ds(row, TILE)] = value
        if self.wraps:
            if row == self.rows[0]:
                ref[p, c, pl.ds(self.rows[-1] + TILE, 1)] = value[:1]
            if row == self.rows[-1]:
                ref[p, c, pl.ds(self.rows[0] - 1, 1)] = value[TILE - 1 :]

    def wrap(self, ref):
        def body(p):
            for c in range(ref.shape[1]):
                end = self.rows[-1] + TILE
                ref[p, c, pl.ds(end, 1)] = ref[p, c, pl.ds(self.rows[0], 1)]
                ref[p, c, pl.ds(self.rows[0] - 1, 1)] = ref[p, c, pl.ds(end - 1, 1)]

        loop(ref.shape[0], body, 4)

    def second(self, u, new, planes, steps):
        start = coefficients(steps)[0][1]
        keep, gain = coefficients(steps)[1]
        mine, theirs = keep * start + gain * (1.0 - start), gain * start

        def body(p):
            for row in self.rows:
                here, beside = beside_of(u, p, row)
                for c in range(len(here)):
                    change = mine * here[c] + theirs * (rows_at(self.m, p, c, row) * beside[c])
                    self.d[p, c, pl.ds(row, TILE)] = change
                    self.put(new, p, c, row, start * here[c] + change)

        self.run(planes, body)

    def step(self, u, old, new, planes, pair, save=True, plus=None):
        keep, gain = pair

        def body(p):
            for row in self.rows:
                here, beside = beside_of(old, p, row)
                for c in range(len(here)):
                    pull = rows_at(self.m, p, c, row) * beside[c] + rows_at(u, p, c, row)
                    change = gain * (pull - here[c])
                    if keep:
                        change = keep * rows_at(self.d, p, c, row) + change
                    if save:
                        self.d[p, c, pl.ds(row, TILE)] = change
                    value = here[c] + change
                    if plus is not None:
                        value = value + rows_at(plus, p, c, row)
                    self.put(new, p, c, row, value)

        self.run(planes, body)

    def residual(self, u, w, out, planes, rows):
        def body(p):
            for row in rows:
                here, beside = beside_of(w, p, row)
                for c in range(len(here)):
                    pull = (rows_at(u, p, c, row) - here[c]) * rows_at(self.g, p, c, row)
                    out[p, c, pl.ds(row, TILE)] = pull + beside[c]

        self.run(planes, body)


def coarsen(fine, coarse, planes, rows, factor, m=None):
    def body(p):
        for c in range(coarse.shape[1]):
            for row in range(0, rows, TILE):
                total = None
                for half in range(2):
                    for chunk in (2 * c, 2 * c + 1):
                        for odd in range(2):
                            at = pl.ds(PAD + 2 * row + odd, TILE, stride=2)
                            term = fine[2 * p + half, chunk, at]
                            total = term if total is None else total + term
                total = total * factor
                if m is not None:
                    total = total * rows_at(m, p, c, PAD + row)
                coarse[p, c, pl.ds(PAD + row, TILE)] = total

    loop(planes, body, 2)


def kernel(sizes, z_window, pairs, source, conduct, adjoint, residual,
           raw_f, raw_k, f0, k0, m0, g0, inv0, u0a, u0b, wa0, wb0, d0, ha, hb, ws, t0,
           k1, m1, g1, inv1, u1a, u1b, wa1, wb1, d1, t1, e0,
           k2, m2, g2, inv2, u2, wa2, wb2, d2, e1,
           load_sem, send_sem, recv_sem):
    gz, gy = sizes
    own_z, own_y, nx = source.shape
    mz, my = own_z // 2, own_y // 2
    zs = k0.shape[0]
    mid_planes, low_planes = k1.shape[0], k2.shape[0]
    mid_rows, low_rows = k1.shape[2] - 2 * PAD, k2.shape[2] - 2 * PAD
    me_z, me_y = lax.axis_index("gz"), lax.axis_index("gy")
    core = lax.rem(me_y, 2)
    mate = 1 - 2 * core
    slots = 2 * len(pairs)

    def at(oz, oy):
        return (lax.rem(me_z + oz + gz, gz), lax.rem(me_y + oy + gy, gy))

    load_k = pltpu.make_async_copy(conduct, raw_k, load_sem.at[0])
    load_f = pltpu.make_async_copy(source, raw_f, load_sem.at[1])
    load_k.start()
    load_f.start()

    barrier = pltpu.get_barrier_semaphore()
    near = [-1, 0, 1]
    greet = {(oz % gz, oy % gy) for oz in near for oy in near}
    for s in z_window:
        greet |= {(s % gz, 0), (-s % gz, 0)}
    for s in pairs:
        greet |= {(0, 2 * s % gy), (0, -2 * s % gy)}
    greet = sorted(greet - {(0, 0)})
    for oz, oy in greet:
        pl.semaphore_signal(barrier, inc=1, device_id=at(oz, oy), device_id_type=MESH)

    share = nx // LANES

    def deal(r, c, value):
        pick = r == share * (c & (LANES - 1)) + c // LANES
        return jnp.where(pick, value, 0.0).astype(jnp.bfloat16)

    rows = lax.broadcasted_iota(jnp.int32, (nx, nx), 0)
    columns = lax.broadcasted_iota(jnp.int32, (nx, nx), 1)

    def enter(raw, out, row, value):
        flat = pick_columns(raw[...].reshape(own_z * own_y, nx), deal(rows, columns, value), 3)
        for p in range(own_z):
            for c in range(share):
                piece = flat[p * own_y : (p + 1) * own_y, c * LANES : (c + 1) * LANES]
                out[p, c, pl.ds(row, own_y)] = piece

    own_tiles = tuple(range(PAD, PAD + own_y, TILE))
    fine_tiles = tuple(range(PAD - HALO, PAD + own_y + HALO, TILE))
    fine = Level(k0, m0, g0, inv0, d0, wa0, wb0, fine_tiles, False, 2)
    mid = Level(k1, m1, g1, inv1, d1, wa1, wb1, tuple(range(PAD, PAD + mid_rows, TILE)), True, 2)
    low = Level(k2, m2, g2, inv2, d2, wa2, wb2, tuple(range(PAD, PAD + low_rows, TILE)), True, 8)

    def around(margin):
        return (zs - margin, own_z + 2 * margin)

    def weigh(level, p, row, whole=True):
        for c in range(level.k.shape[1]):
            inverse = 1.0 / rows_at(level.k, p, c, row)
            g = 6.0 + inverse
            level.m[p, c, pl.ds(row, TILE)] = 1.0 / g
            if whole:
                level.g[p, c, pl.ds(row, TILE)] = g
                level.inverse[p, c, pl.ds(row, TILE)] = inverse

    load_k.wait()
    enter(raw_k, k0, PAD, heat_step)

    def own_weights(p):
        for row in own_tiles:
            weigh(fine, p, row)

    loop(own_z, own_weights)
    load_f.wait()
    enter(raw_f, f0, 0, 1.0)

    def own_start(p):
        for c in range(share):
            for row in own_tiles:
                value = rows_at(m0, p, c, row) * rows_at(f0, p, c, row - PAD)
                u0a[p, c, pl.ds(row, TILE)] = value

    loop(own_z, own_start)
    coarsen(k0, k1, mz, my, 0.125 / 4.0)

    def own_mid_weights(p):
        for row in range(PAD, PAD + my, TILE):
            weigh(mid, p, row)

    loop(mz, own_mid_weights)

    pl.semaphore_wait(barrier, len(greet))

    counts = {"send": 0, "recv": 0}
    unsent = []

    def take(kind):
        counts[kind] += 1
        sems = send_sem if kind == "send" else recv_sem
        return sems.at[counts[kind] - 1]

    def copy_of(from_ref, to_ref, sent, got, device):
        return pltpu.make_async_remote_copy(
            src_ref=from_ref, dst_ref=to_ref, send_sem=sent, recv_sem=got,
            device_id=device, device_id_type=MESH)

    def send(from_ref, to_ref, device):
        copy = copy_of(from_ref, to_ref, take("send"), take("recv"), device)
        copy.start()
        unsent.append(copy)
        return copy

    odd = lax.rem(me_z, 2)
    sides = [2 * odd - 1, 1 - 2 * odd]

    def face(own, held, side, skip, depth, row_side, depth_y, device):
        up = side > 0
        count = depth - skip
        start = jnp.where(up, own_z - depth, skip)
        land = jnp.where(up, zs - depth, own_z + skip)
        if row_side == 0:
            row, to_row, height = PAD, PAD, own_y
        elif row_side > 0:
            row, to_row, height = PAD + own_y - depth_y, PAD - depth_y, depth_y
        else:
            row, to_row, height = PAD, PAD + own_y, depth_y
        return send(own.at[pl.ds(start, count), :, pl.ds(row, height)],
                    held.at[pl.ds(land, count), :, pl.ds(to_row, height)], device)

    def flank(own, held, row_side, depth_y):
        planes = pl.ds(0, own_z)
        if row_side > 0:
            row, to_row = PAD + own_y - depth_y, PAD - depth_y
        else:
            row, to_row = PAD, PAD + own_y
        return send(own.at[planes, :, pl.ds(row, depth_y)],
                    held.at[planes, :, pl.ds(to_row, depth_y)], at(0, row_side))

    def surround(jobs):
        copies = []
        for number, side in enumerate(sides):
            for ref, depth, depth_y, corner, corner_y in jobs:
                copies.append(face(ref, ref, side, 0, depth, 0, 0, at(side, 0)))
            for ref, depth, depth_y, corner, corner_y in jobs:
                for row_side in (1, -1):
                    copies.append(face(ref, ref, side, 0, corner, row_side, corner_y,
                                       at(side, row_side)))
            if number == 0:
                for ref, depth, depth_y, corner, corner_y in jobs:
                    for row_side in (1, -1):
                        copies.append(flank(ref, ref, row_side, depth_y))
        return copies

    def beyond(ref):
        copies = []
        for side in sides:
            copies.append(face(ref, ref, side, 2, HALO, 0, 0, at(side, 0)))
            for row_side in (1, -1):
                copies.append(face(ref, ref, side, 2, HALO - 1, row_side, 1, at(side, row_side)))
        return copies

    def await_all(copies):
        for copy in copies:
            copy.wait_recv()

    far_first = sorted(range(len(z_window)), key=lambda s: -abs(z_window[s]))[:-1]

    class Gather:
        def __init__(self, held):
            self.held = held
            self.z = {}
            for s in far_first:
                self.z[s] = send(self.block(0, 0), self.block(s, 0), at(-z_window[s], 0))
            self.y = {n: (take("send"), take("recv")) for n in range(1, len(pairs))}
            self.spread(0)

        def rows(self, slot):
            return pl.ds(pl.multiple_of(PAD + slot * my, TILE), my)

        def block(self, s, slot):
            return self.held.at[pl.ds(s * mz, mz), :, self.rows(slot)]

        def column(self, slot):
            return self.held.at[:, :, self.rows(slot)]

        def spread(self, s):
            for n in range(1, len(pairs)):
                slot = 2 * pairs[n] % slots
                sent, got = self.y[n]
                copy_of(self.block(s, 0), self.block(s, slot), sent, got,
                        at(0, -2 * pairs[n])).start()

        def mirror(self, n):
            slot = 2 * pairs[n] % slots
            to_slot = lax.rem(slot - mate + slots, slots)
            return send(self.column(slot), self.column(to_slot), at(0, mate))

        def forward(self):
            for s in far_first:
                self.z[s].wait_recv()
                self.spread(s)
            self.mate = [self.mirror(0)]

        def across(self):
            for n in range(1, len(pairs)):
                slot = 2 * pairs[n] % slots
                whole = copy_of(self.column(0), self.column(slot), *self.y[n],
                                at(0, -2 * pairs[n]))
                whole.wait_recv()
                unsent.append(whole)
                self.mate.append(self.mirror(n))

        def wait(self):
            await_all(self.mate)

    first = surround([(u0a, 3, 3, 2, 2), (k0, 2, HALO, 2, 3)])
    gather_k = Gather(k1)
    await_all(first)

    steps = coefficients(DEGREE)

    def weights(p):
        for row in fine_tiles:
            weigh(fine, p, row, False)

    def some_weights(start, count):
        loop(count, lambda i: weights(lax.rem(i + start, zs)))

    some_weights(0, own_z + 2)
    some_weights(zs - 2, 2)

    def down(u, held, u1, between=None):
        fine.second(u, wa0, around(2), DEGREE)
        if between:
            between()
        fine.step(u, wa0, wb0, around(1), steps[2], save=False)
        fine.residual(u, wb0, t0, (0, own_z), own_tiles)
        coarsen(t0, u1, mz, my, 0.125, m1)
        gather = Gather(u1)

        def hold(p):
            for c in range(share):
                for row in own_tiles:
                    held[p, c, pl.ds(row, TILE)] = rows_at(wb0, p, c, row)

        loop(own_z, hold)
        return gather

    def solve(u1):
        everywhere = (0, mid_planes)
        mid.wrap(u1)
        mid.second(u1, wa1, everywhere, DEGREE)
        mid.step(u1, wa1, wb1, everywhere, steps[2], save=False)
        mid.residual(u1, wb1, t1, everywhere, mid.rows)
        coarsen(t1, u2, low_planes, low_rows, 0.125, m2)
        low.wrap(u2)
        low_steps = coefficients(COARSE_DEGREE)
        deep = (0, low_planes)
        low.second(u2, wa2, deep, COARSE_DEGREE)
        low.step(u2, wa2, wb2, deep, low_steps[2])
        low.step(u2, wb2, wa2, deep, low_steps[3], save=False)
        margin = HALO // 2 + DEGREE
        pairs_first, pairs_count = -(-margin // 2), mz // 2 + 2 * -(-margin // 2)
        pairs_count = min(pairs_count, low_planes)

        def lift(i):
            p = lax.rem(i + low_planes - pairs_first, low_planes)
            for row in low.rows:
                value = rows_at(wa2, p, 0, row) * rows_at(inv2, p, 0, row)
                spot = PAD + 2 * (row - PAD)
                for o in range(2):
                    e1[p, 0, pl.ds(spot + o, TILE, stride=2)] = value

        loop(pairs_count, lift)

        def add(i):
            p = lax.rem(i + low_planes - pairs_first, low_planes)
            for half in range(2):
                q = 2 * p + half
                for c in range(k1.shape[1]):
                    for row in mid.rows:
                        value = rows_at(wb1, q, c, row)
                        value = value + rows_at(k1, q, c, row) * rows_at(e1, p, c // 2, row)
                        mid.put(wb1, q, c, row, value)

        loop(pairs_count, add, 1)

        def near_own(reach):
            if mz + 2 * reach >= mid_planes:
                return everywhere
            return (mid_planes - reach, mz + 2 * reach)

        reach = HALO // 2
        mid.step(u1, wb1, wa1, near_own(reach + 2), steps[0])
        mid.step(u1, wa1, wb1, near_own(reach + 1), steps[1])
        mid.step(u1, wb1, wa1, near_own(reach), steps[2], save=False)

        def lift_fine(i):
            q = lax.rem(i + mid_planes - reach, mid_planes)
            for c in range(k1.shape[1]):
                for row in range(-TILE, my + TILE, TILE):
                    here = PAD + row % mid_rows
                    value = rows_at(wa1, q, c, here) * rows_at(inv1, q, c, here)
                    for o in range(2):
                        e0[i, c, pl.ds(EDGE + 2 * row + o, TILE, stride=2)] = value

        loop(mz + 2 * reach, lift_fine)

    def up(u, held, out, plus=None):
        reach = HALO // 2

        def body(i):
            for half in range(2):
                p = lax.rem(2 * i + half + zs - HALO, zs)
                for c in range(share):
                    for row in fine_tiles:
                        add = rows_at(e0, i, c // 2, EDGE + row - PAD)
                        value = rows_at(held, p, c, row) + rows_at(k0, p, c, row) * add
                        wa0[p, c, pl.ds(row, TILE)] = value

        loop(mz + 2 * reach, body, 1)
        fine.step(u, wa0, wb0, around(3), steps[0])
        fine.step(u, wb0, wa0, around(2), steps[1])
        fine.step(u, wa0, out, around(1), steps[2], save=False, plus=plus)

    def remain(p, row, w):
        here, beside = beside_of(w, p, row)
        values = []
        for c in range(share):
            pull = rows_at(f0, p, c, row - PAD) - rows_at(g0, p, c, row) * here[c]
            values.append(pull + beside[c])
        return here, values

    gather = down(u0a, ha, u1a, gather_k.forward)
    gather_k.across()
    more = beyond(k0)
    gather.forward()
    held = surround([(ha, HALO, HALO, 3, 3)])
    gather_k.wait()

    def mid_weights(p):
        for row in mid.rows:
            weigh(mid, p, row)

    loop(mid_planes, mid_weights)
    coarsen(k1, k2, low_planes, low_rows, 0.125 / 4.0)

    def low_weights(p):
        for row in low.rows:
            weigh(low, p, row)

    loop(low_planes, low_weights, 4)
    gather.across()
    gather.wait()
    solve(u1a)
    await_all(more)
    some_weights(own_z + 2, 1)
    some_weights(zs - 3, 1)
    await_all(held)
    up(u0a, ha, ws)

    def again(p):
        for row in own_tiles:
            _, values = remain(p, row, ws)
            for c in range(share):
                u0b[p, c, pl.ds(row, TILE)] = rows_at(m0, p, c, row) * values[c]

    loop(own_z, again)
    second = surround([(u0b, 3, 3, 2, 2)])
    await_all(second)
    gather = down(u0b, hb, u1b)
    gather.forward()
    held = surround([(hb, HALO, HALO, 3, 3)])
    gather.across()
    gather.wait()
    solve(u1b)
    await_all(held)
    up(u0b, hb, wb0, plus=ws)

    back = deal(columns, rows, 1.0)

    def leave(pieces, out):
        flat = jnp.concatenate(pieces, axis=1)
        out[...] = pick_columns(flat, back, 2).reshape(own_z, own_y, nx)

    def finish(p):
        for row in own_tiles:
            _, values = remain(p, row, wb0)
            for c in range(share):
                t0[p, c, pl.ds(row, TILE)] = values[c]

    loop(own_z, finish)

    def pieces_of(ref, weight=None):
        pieces = []
        for c in range(share):
            parts = []
            for p in range(own_z):
                value = ref[p, c, pl.ds(PAD, own_y)]
                if weight is not None:
                    value = value * weight[p, c, pl.ds(PAD, own_y)]
                parts.append(value)
            pieces.append(jnp.concatenate(parts, axis=0))
        return pieces

    leave(pieces_of(wb0, inv0), adjoint)
    leave(pieces_of(t0), residual)
    for copy in unsent:
        copy.wait_send()
    assert counts["send"] <= send_sem.shape[0] and counts["recv"] <= recv_sem.shape[0], counts


def local(sizes, source, conduct):
    own_z, own_y, nx = source.shape
    z_window = window(sizes[0], -(-MID_REACH // (own_z // 2)))
    pairs = window(sizes[1] // 2, -(-MID_REACH // own_y))
    chunks = nx // LANES
    mz, my = own_z // 2, own_y // 2
    mid_planes, mid_rows = len(z_window) * mz, 2 * len(pairs) * my
    fine = (own_z + 2 * HALO, chunks, own_y + 2 * PAD, LANES)
    mid = (mid_planes, chunks // 2, mid_rows + 2 * PAD, LANES)
    low = (mid_planes // 2, chunks // 4, mid_rows // 2 + 2 * PAD, LANES)
    lifted = (mz + HALO, chunks // 2, own_y + 2 * EDGE, LANES)
    lifted_low = (mid_planes // 2, chunks // 4, mid_rows + 2 * PAD, LANES)
    inside = (own_z, chunks, own_y, LANES)
    vmem = lambda shape, count: [pltpu.VMEM(shape, jnp.float32)] * count
    gathers = 3 * (len(z_window) - 1 + 2 * len(pairs) - 1)
    copies = 5 * 8 + 6 + gathers
    return pl.pallas_call(
        functools.partial(kernel, sizes, z_window, pairs),
        out_shape=[pltpu.VMEM(source.shape, jnp.float32)] * 2,
        in_specs=[pl.BlockSpec(memory_space=pl.ANY)] * 2,
        out_specs=[pl.BlockSpec(memory_space=pltpu.VMEM)] * 2,
        scratch_shapes=vmem(source.shape, 2) + vmem(inside, 1) + vmem(fine, 13)
        + vmem(mid, 10) + vmem(lifted, 1) + vmem(low, 8) + vmem(lifted_low, 1) + [
            pltpu.SemaphoreType.DMA((2,)),
            pltpu.SemaphoreType.DMA((copies,)),
            pltpu.SemaphoreType.DMA((copies,)),
        ],
        compiler_params=pltpu.CompilerParams(
            collective_id=0, has_side_effects=True, vmem_limit_bytes=56 * 1024 * 1024
        ),
    )(source, conduct)


def solution(mesh):
    spec = P("gz", "gy", None)
    sizes = (mesh.shape["gz"], mesh.shape["gy"])
    return jax.shard_map(
        functools.partial(local, sizes),
        mesh=mesh,
        in_specs=(spec, spec),
        out_specs=(spec, spec),
        check_vma=False,
    )
```

```python
import functools

import jax
import jax.numpy as jnp
from jax import lax
from jax.experimental import pallas as pl
from jax.experimental.pallas import tpu as pltpu
from jax.sharding import PartitionSpec as P

DEGREE = 3
COARSE_DEGREE = 4

cheb_low = 0.3
cheb_high = 1.9
heat_step = 4.0

HALO = 4
PAD = 8
EDGE = 16
MID_REACH = 15
MESH = pl.DeviceIdType.MESH
LANES = 128
TILE = 8


def coefficients(steps):
    theta = (cheb_high + cheb_low) / 2.0
    delta = (cheb_high - cheb_low) / 2.0
    sigma = theta / delta
    rho = 1.0 / sigma
    pairs = [(0.0, 1.0 / theta)]
    for _ in range(steps - 1):
        rho_next = 1.0 / (2.0 * sigma - rho)
        pairs.append((rho_next * rho, 2.0 * rho_next / delta))
        rho = rho_next
    return pairs


def window(devices, reach):
    count = min(2 * reach + 1, devices)
    ahead = count // 2
    return [s if s <= ahead else s - count for s in range(count)]


def parts_of(value, count):
    parts = []
    for _ in range(count):
        parts.append(value.astype(jnp.bfloat16))
        value = value - parts[-1].astype(jnp.float32)
    return parts


def pick_columns(value, columns, count):
    total = None
    for part in reversed(parts_of(value, count)):
        term = jnp.dot(part, columns, preferred_element_type=jnp.float32)
        total = term if total is None else total + term
    return total


def unrolled(count, most):
    return max(u for u in range(1, most + 1) if count % u == 0)


def loop(count, body, most=16):
    def step(i, carry):
        body(i)
        return carry

    lax.fori_loop(0, count, step, 0, unroll=unrolled(count, most))


def rows_at(ref, p, c, row):
    return ref[p, c, pl.ds(row, TILE)]


def beside_of(w, p, row):
    planes, chunks = w.shape[0], w.shape[1]
    after, before = lax.rem(p + 1, planes), lax.rem(p + planes - 1, planes)
    here = [rows_at(w, p, c, row) for c in range(chunks)]
    lane = lax.broadcasted_iota(jnp.int32, here[0].shape, 1)
    first = jnp.where(lane == 0, 0.0, pltpu.roll(here[-1], 1, 1))
    last = jnp.where(lane == LANES - 1, 0.0, pltpu.roll(here[0], LANES - 1, 1))
    around = [first] + here + [last]
    beside = []
    for c in range(chunks):
        total = rows_at(w, after, c, row) + rows_at(w, before, c, row)
        total = total + (rows_at(w, p, c, row - 1) + rows_at(w, p, c, row + 1))
        beside.append(total + (around[c] + around[c + 2]))
    return here, beside


class Level:
    def __init__(self, k, m, g, inverse, d, wa, wb, rows, wraps):
        self.k, self.m, self.g, self.inverse, self.d = k, m, g, inverse, d
        self.w = (wa, wb)
        self.rows, self.wraps = rows, wraps

    def run(self, planes, body):
        first, count = planes

        def at(i):
            body(lax.rem(i + first, self.k.shape[0]))

        loop(count, at)

    def put(self, ref, p, c, row, value):
        ref[p, c, pl.ds(row, TILE)] = value
        if self.wraps:
            if row == self.rows[0]:
                ref[p, c, pl.ds(self.rows[-1] + TILE, 1)] = value[:1]
            if row == self.rows[-1]:
                ref[p, c, pl.ds(self.rows[0] - 1, 1)] = value[TILE - 1 :]

    def wrap(self, ref):
        def body(p):
            for c in range(ref.shape[1]):
                end = self.rows[-1] + TILE
                ref[p, c, pl.ds(end, 1)] = ref[p, c, pl.ds(self.rows[0], 1)]
                ref[p, c, pl.ds(self.rows[0] - 1, 1)] = ref[p, c, pl.ds(end - 1, 1)]

        loop(ref.shape[0], body)

    def second(self, u, new, planes, steps):
        start = coefficients(steps)[0][1]
        keep, gain = coefficients(steps)[1]
        mine, theirs = keep * start + gain * (1.0 - start), gain * start

        def body(p):
            for row in self.rows:
                here, beside = beside_of(u, p, row)
                for c in range(len(here)):
                    change = mine * here[c] + theirs * (rows_at(self.m, p, c, row) * beside[c])
                    self.d[p, c, pl.ds(row, TILE)] = change
                    self.put(new, p, c, row, start * here[c] + change)

        self.run(planes, body)

    def step(self, u, old, new, planes, pair, save=True, plus=None):
        keep, gain = pair

        def body(p):
            for row in self.rows:
                here, beside = beside_of(old, p, row)
                for c in range(len(here)):
                    pull = rows_at(self.m, p, c, row) * beside[c] + rows_at(u, p, c, row)
                    change = gain * (pull - here[c])
                    if keep:
                        change = keep * rows_at(self.d, p, c, row) + change
                    if save:
                        self.d[p, c, pl.ds(row, TILE)] = change
                    value = here[c] + change
                    if plus is not None:
                        value = value + rows_at(plus, p, c, row)
                    self.put(new, p, c, row, value)

        self.run(planes, body)

    def residual(self, u, w, out, planes, rows):
        def body(p):
            for row in rows:
                here, beside = beside_of(w, p, row)
                for c in range(len(here)):
                    pull = (rows_at(u, p, c, row) - here[c]) * rows_at(self.g, p, c, row)
                    out[p, c, pl.ds(row, TILE)] = pull + beside[c]

        self.run(planes, body)


def coarsen(fine, coarse, planes, rows, factor, m=None):
    def body(p):
        for c in range(coarse.shape[1]):
            for row in range(0, rows, TILE):
                total = None
                for half in range(2):
                    for chunk in (2 * c, 2 * c + 1):
                        for odd in range(2):
                            at = pl.ds(PAD + 2 * row + odd, TILE, stride=2)
                            term = fine[2 * p + half, chunk, at]
                            total = term if total is None else total + term
                total = total * factor
                if m is not None:
                    total = total * rows_at(m, p, c, PAD + row)
                coarse[p, c, pl.ds(PAD + row, TILE)] = total

    loop(planes, body)


def kernel(sizes, z_window, pairs, source, conduct, adjoint, residual,
           raw_f, raw_k, f0, k0, m0, g0, inv0, u0a, u0b, wa0, wb0, d0, ha, hb, ws, t0,
           k1, m1, g1, inv1, u1a, u1b, wa1, wb1, d1, t1, e0,
           k2, m2, g2, inv2, u2, wa2, wb2, d2, e1,
           load_sem, send_sem, recv_sem):
    gz, gy = sizes
    own_z, own_y, nx = source.shape
    mz, my = own_z // 2, own_y // 2
    zs = k0.shape[0]
    mid_planes, low_planes = k1.shape[0], k2.shape[0]
    mid_rows, low_rows = k1.shape[2] - 2 * PAD, k2.shape[2] - 2 * PAD
    me_z, me_y = lax.axis_index("gz"), lax.axis_index("gy")
    core = lax.rem(me_y, 2)
    mate = 1 - 2 * core
    slots = 2 * len(pairs)

    def at(oz, oy):
        return (lax.rem(me_z + oz + gz, gz), lax.rem(me_y + oy + gy, gy))

    load_k = pltpu.make_async_copy(conduct, raw_k, load_sem.at[0])
    load_f = pltpu.make_async_copy(source, raw_f, load_sem.at[1])
    load_k.start()
    load_f.start()

    barrier = pltpu.get_barrier_semaphore()
    near = [-1, 0, 1]
    greet = {(oz % gz, oy % gy) for oz in near for oy in near}
    for s in z_window:
        greet |= {(s % gz, 0), (-s % gz, 0)}
    for s in pairs:
        greet |= {(0, 2 * s % gy), (0, -2 * s % gy)}
    greet = sorted(greet - {(0, 0)})
    for oz, oy in greet:
        pl.semaphore_signal(barrier, inc=1, device_id=at(oz, oy), device_id_type=MESH)

    share = nx // LANES

    def deal(r, c, value):
        pick = r == share * (c & (LANES - 1)) + c // LANES
        return jnp.where(pick, value, 0.0).astype(jnp.bfloat16)

    rows = lax.broadcasted_iota(jnp.int32, (nx, nx), 0)
    columns = lax.broadcasted_iota(jnp.int32, (nx, nx), 1)

    def enter(raw, out, row, value):
        flat = pick_columns(raw[...].reshape(own_z * own_y, nx), deal(rows, columns, value), 3)
        for p in range(own_z):
            for c in range(share):
                piece = flat[p * own_y : (p + 1) * own_y, c * LANES : (c + 1) * LANES]
                out[p, c, pl.ds(row, own_y)] = piece

    own_tiles = tuple(range(PAD, PAD + own_y, TILE))
    fine_tiles = tuple(range(PAD - HALO, PAD + own_y + HALO, TILE))
    fine = Level(k0, m0, g0, inv0, d0, wa0, wb0, fine_tiles, False)
    mid = Level(k1, m1, g1, inv1, d1, wa1, wb1, tuple(range(PAD, PAD + mid_rows, TILE)), True)
    low = Level(k2, m2, g2, inv2, d2, wa2, wb2, tuple(range(PAD, PAD + low_rows, TILE)), True)

    def around(margin):
        return (zs - margin, own_z + 2 * margin)

    def weigh(level, p, row, whole=True):
        for c in range(level.k.shape[1]):
            inverse = 1.0 / rows_at(level.k, p, c, row)
            g = 6.0 + inverse
            level.m[p, c, pl.ds(row, TILE)] = 1.0 / g
            if whole:
                level.g[p, c, pl.ds(row, TILE)] = g
                level.inverse[p, c, pl.ds(row, TILE)] = inverse

    load_k.wait()
    enter(raw_k, k0, PAD, heat_step)

    def own_weights(p):
        for row in own_tiles:
            weigh(fine, p, row)

    loop(own_z, own_weights)
    load_f.wait()
    enter(raw_f, f0, 0, 1.0)

    def own_start(p):
        for c in range(share):
            for row in own_tiles:
                value = rows_at(m0, p, c, row) * rows_at(f0, p, c, row - PAD)
                u0a[p, c, pl.ds(row, TILE)] = value

    loop(own_z, own_start)
    coarsen(k0, k1, mz, my, 0.125 / 4.0)

    def own_mid_weights(p):
        for row in range(PAD, PAD + my, TILE):
            weigh(mid, p, row)

    loop(mz, own_mid_weights)

    pl.semaphore_wait(barrier, len(greet))

    counts = {"send": 0, "recv": 0}
    unsent = []

    def take(kind):
        counts[kind] += 1
        sems = send_sem if kind == "send" else recv_sem
        return sems.at[counts[kind] - 1]

    def copy_of(from_ref, to_ref, sent, got, device):
        return pltpu.make_async_remote_copy(
            src_ref=from_ref, dst_ref=to_ref, send_sem=sent, recv_sem=got,
            device_id=device, device_id_type=MESH)

    def send(from_ref, to_ref, device):
        copy = copy_of(from_ref, to_ref, take("send"), take("recv"), device)
        copy.start()
        unsent.append(copy)
        return copy

    odd = lax.rem(me_z, 2)
    sides = [2 * odd - 1, 1 - 2 * odd]

    def face(own, held, side, skip, depth, row_side, depth_y, device):
        up = side > 0
        count = depth - skip
        start = jnp.where(up, own_z - depth, skip)
        land = jnp.where(up, zs - depth, own_z + skip)
        if row_side == 0:
            row, to_row, height = PAD, PAD, own_y
        elif row_side > 0:
            row, to_row, height = PAD + own_y - depth_y, PAD - depth_y, depth_y
        else:
            row, to_row, height = PAD, PAD + own_y, depth_y
        return send(own.at[pl.ds(start, count), :, pl.ds(row, height)],
                    held.at[pl.ds(land, count), :, pl.ds(to_row, height)], device)

    def flank(own, held, row_side, skip, depth_y):
        planes, height = pl.ds(0, own_z), depth_y - skip
        if row_side > 0:
            row, to_row = PAD + own_y - depth_y, PAD - depth_y
        else:
            row, to_row = PAD + skip, PAD + own_y + skip
        return send(own.at[planes, :, pl.ds(row, height)],
                    held.at[planes, :, pl.ds(to_row, height)], at(0, row_side))

    def surround(jobs):
        copies = []
        for number, side in enumerate(sides):
            for ref, skip, depth, depth_y, corners in jobs:
                copies.append(face(ref, ref, side, skip, depth, 0, 0, at(side, 0)))
            for ref, skip, depth, depth_y, corners in jobs:
                for row_side in (1, -1):
                    for n, corner in enumerate(corners):
                        copies.append(face(ref, ref, side, n, n + 1, row_side, corner,
                                           at(side, row_side)))
            if number == 0:
                for ref, skip, depth, depth_y, corners in jobs:
                    for row_side in (1, -1):
                        copies.append(flank(ref, ref, row_side, skip, depth_y))
        return copies

    def beyond(ref):
        copies = [face(ref, ref, sides[1], 2, HALO, 0, 0, at(sides[1], 0))]
        for side in sides:
            for row_side in (1, -1):
                copies.append(face(ref, ref, side, 2, HALO - 1, row_side, 1, at(side, row_side)))
        return copies

    def relay(ref):
        up = sides[1] > 0
        start = jnp.where(up, own_z, zs - 2)
        land = jnp.where(up, zs - HALO, own_z + 2)
        own_rows = pl.ds(PAD, own_y)
        return [send(ref.at[pl.ds(start, 2), :, own_rows], ref.at[pl.ds(land, 2), :, own_rows],
                     at(2 * sides[1], 0))]

    def await_all(copies):
        for copy in copies:
            copy.wait_recv()

    far_first = sorted(range(len(z_window)), key=lambda s: -abs(z_window[s]))[:-1]

    class Gather:
        def __init__(self, held):
            self.held = held
            self.z = {}
            for s in far_first:
                self.z[s] = send(self.block(0, 0), self.block(s, 0), at(-z_window[s], 0))
            self.y = {n: (take("send"), take("recv")) for n in range(1, len(pairs))}
            self.spread(0)

        def rows(self, slot):
            return pl.ds(pl.multiple_of(PAD + slot * my, TILE), my)

        def block(self, s, slot):
            return self.held.at[pl.ds(s * mz, mz), :, self.rows(slot)]

        def column(self, slot):
            return self.held.at[:, :, self.rows(slot)]

        def spread(self, s):
            for n in range(1, len(pairs)):
                slot = 2 * pairs[n] % slots
                sent, got = self.y[n]
                copy_of(self.block(s, 0), self.block(s, slot), sent, got,
                        at(0, -2 * pairs[n])).start()

        def mirror(self, n):
            slot = 2 * pairs[n] % slots
            to_slot = lax.rem(slot - mate + slots, slots)
            return send(self.column(slot), self.column(to_slot), at(0, mate))

        def forward(self):
            for s in far_first:
                self.z[s].wait_recv()
                self.spread(s)
            self.mate = [self.mirror(0)]

        def across(self):
            for n in range(1, len(pairs)):
                slot = 2 * pairs[n] % slots
                whole = copy_of(self.column(0), self.column(slot), *self.y[n],
                                at(0, -2 * pairs[n]))
                whole.wait_recv()
                unsent.append(whole)
                self.mate.append(self.mirror(n))

        def wait(self):
            await_all(self.mate)

    first = surround([(u0a, 0, 3, 3, (2, 1)), (k0, 0, 2, HALO, (3, 2))])
    gather_k = Gather(k1)
    more = beyond(k0)
    await_all(first)
    more += relay(k0)

    steps = coefficients(DEGREE)

    def weights(p):
        for row in fine_tiles:
            weigh(fine, p, row, False)

    def some_weights(start, count):
        loop(count, lambda i: weights(lax.rem(i + start, zs)))

    some_weights(0, own_z + 2)
    some_weights(zs - 2, 2)

    def down(u, held, u1, between=None):
        fine.second(u, wa0, around(2), DEGREE)
        if between:
            between()
        fine.step(u, wa0, wb0, around(1), steps[2], save=False)
        fine.residual(u, wb0, t0, (0, own_z), own_tiles)
        coarsen(t0, u1, mz, my, 0.125, m1)
        gather = Gather(u1)

        def hold(p, edges=True):
            for c in range(share):
                for row in own_tiles:
                    held[p, c, pl.ds(row, TILE)] = rows_at(wb0, p, c, row)
                if edges:
                    for row in (PAD - 1, PAD + own_y):
                        held[p, c, pl.ds(row, 1)] = wb0[p, c, pl.ds(row, 1)]

        loop(own_z, hold)
        for p in (own_z, zs - 1):
            hold(p, False)
        return gather

    def solve(u1):
        everywhere = (0, mid_planes)
        mid.wrap(u1)
        mid.second(u1, wa1, everywhere, DEGREE)
        mid.step(u1, wa1, wb1, everywhere, steps[2], save=False)
        mid.residual(u1, wb1, t1, everywhere, mid.rows)
        coarsen(t1, u2, low_planes, low_rows, 0.125, m2)
        low.wrap(u2)
        low_steps = coefficients(COARSE_DEGREE)
        deep = (0, low_planes)
        low.second(u2, wa2, deep, COARSE_DEGREE)
        low.step(u2, wa2, wb2, deep, low_steps[2])
        low.step(u2, wb2, wa2, deep, low_steps[3], save=False)
        margin = HALO // 2 + DEGREE
        pairs_first, pairs_count = -(-margin // 2), mz // 2 + 2 * -(-margin // 2)
        pairs_count = min(pairs_count, low_planes)

        def lift(i):
            p = lax.rem(i + low_planes - pairs_first, low_planes)
            for row in low.rows:
                value = rows_at(wa2, p, 0, row) * rows_at(inv2, p, 0, row)
                spot = PAD + 2 * (row - PAD)
                for o in range(2):
                    e1[p, 0, pl.ds(spot + o, TILE, stride=2)] = value

        loop(pairs_count, lift)

        def add(i):
            p = lax.rem(i + low_planes - pairs_first, low_planes)
            for half in range(2):
                q = 2 * p + half
                for c in range(k1.shape[1]):
                    for row in mid.rows:
                        value = rows_at(wb1, q, c, row)
                        value = value + rows_at(k1, q, c, row) * rows_at(e1, p, c // 2, row)
                        mid.put(wb1, q, c, row, value)

        loop(pairs_count, add)

        def near_own(reach):
            if mz + 2 * reach >= mid_planes:
                return everywhere
            return (mid_planes - reach, mz + 2 * reach)

        reach = HALO // 2
        mid.step(u1, wb1, wa1, near_own(reach + 2), steps[0])
        mid.step(u1, wa1, wb1, near_own(reach + 1), steps[1])
        mid.step(u1, wb1, wa1, near_own(reach), steps[2], save=False)

        def lift_fine(i):
            q = lax.rem(i + mid_planes - reach, mid_planes)
            for c in range(k1.shape[1]):
                for row in range(-TILE, my + TILE, TILE):
                    here = PAD + row % mid_rows
                    value = rows_at(wa1, q, c, here) * rows_at(inv1, q, c, here)
                    for o in range(2):
                        e0[i, c, pl.ds(EDGE + 2 * row + o, TILE, stride=2)] = value

        loop(mz + 2 * reach, lift_fine)

    def up(u, held, out, plus=None):
        reach = HALO // 2

        def body(i):
            for half in range(2):
                p = lax.rem(2 * i + half + zs - HALO, zs)
                for c in range(share):
                    for row in fine_tiles:
                        add = rows_at(e0, i, c // 2, EDGE + row - PAD)
                        value = rows_at(held, p, c, row) + rows_at(k0, p, c, row) * add
                        wa0[p, c, pl.ds(row, TILE)] = value

        loop(mz + 2 * reach, body)
        fine.step(u, wa0, wb0, around(3), steps[0])
        fine.step(u, wb0, wa0, around(2), steps[1])
        fine.step(u, wa0, out, around(1), steps[2], save=False, plus=plus)

    def remain(p, row, w):
        here, beside = beside_of(w, p, row)
        values = []
        for c in range(share):
            pull = rows_at(f0, p, c, row - PAD) - rows_at(g0, p, c, row) * here[c]
            values.append(pull + beside[c])
        return here, values

    gather = down(u0a, ha, u1a, gather_k.forward)
    gather_k.across()
    gather.forward()
    held = surround([(ha, 1, HALO, HALO, (3, 2, 1))])
    gather_k.wait()

    def mid_weights(p):
        for row in mid.rows:
            weigh(mid, p, row)

    loop(mid_planes, mid_weights)
    coarsen(k1, k2, low_planes, low_rows, 0.125 / 4.0)

    def low_weights(p):
        for row in low.rows:
            weigh(low, p, row)

    loop(low_planes, low_weights)
    gather.across()
    gather.wait()
    solve(u1a)
    await_all(more)
    some_weights(own_z + 2, 1)
    some_weights(zs - 3, 1)
    await_all(held)
    up(u0a, ha, ws)

    def again(p):
        for row in own_tiles:
            _, values = remain(p, row, ws)
            for c in range(share):
                u0b[p, c, pl.ds(row, TILE)] = rows_at(m0, p, c, row) * values[c]

    loop(own_z, again)
    second = surround([(u0b, 0, 3, 3, (2, 1))])
    await_all(second)
    gather = down(u0b, hb, u1b)
    gather.forward()
    held = surround([(hb, 1, HALO, HALO, (3, 2, 1))])
    gather.across()
    gather.wait()
    solve(u1b)
    await_all(held)
    up(u0b, hb, wb0, plus=ws)

    back = deal(columns, rows, 1.0)

    def leave(pieces, out):
        flat = jnp.concatenate(pieces, axis=1)
        out[...] = pick_columns(flat, back, 2).reshape(own_z, own_y, nx)

    def finish(p):
        for row in own_tiles:
            _, values = remain(p, row, wb0)
            for c in range(share):
                t0[p, c, pl.ds(row, TILE)] = values[c]

    loop(own_z, finish)

    def pieces_of(ref, weight=None):
        pieces = []
        for c in range(share):
            parts = []
            for p in range(own_z):
                value = ref[p, c, pl.ds(PAD, own_y)]
                if weight is not None:
                    value = value * weight[p, c, pl.ds(PAD, own_y)]
                parts.append(value)
            pieces.append(jnp.concatenate(parts, axis=0))
        return pieces

    leave(pieces_of(wb0, inv0), adjoint)
    leave(pieces_of(t0), residual)
    for copy in unsent:
        copy.wait_send()
    assert counts["send"] <= send_sem.shape[0] and counts["recv"] <= recv_sem.shape[0], counts


def local(sizes, source, conduct):
    own_z, own_y, nx = source.shape
    z_window = window(sizes[0], -(-MID_REACH // (own_z // 2)))
    pairs = window(sizes[1] // 2, -(-MID_REACH // own_y))
    chunks = nx // LANES
    mz, my = own_z // 2, own_y // 2
    mid_planes, mid_rows = len(z_window) * mz, 2 * len(pairs) * my
    fine = (own_z + 2 * HALO, chunks, own_y + 2 * PAD, LANES)
    mid = (mid_planes, chunks // 2, mid_rows + 2 * PAD, LANES)
    low = (mid_planes // 2, chunks // 4, mid_rows // 2 + 2 * PAD, LANES)
    lifted = (mz + HALO, chunks // 2, own_y + 2 * EDGE, LANES)
    lifted_low = (mid_planes // 2, chunks // 4, mid_rows + 2 * PAD, LANES)
    inside = (own_z, chunks, own_y, LANES)
    vmem = lambda shape, count: [pltpu.VMEM(shape, jnp.float32)] * count
    gathers = 3 * (len(z_window) - 1 + 2 * len(pairs) - 1)
    copies = 5 * 4 + 4 * (3 * 2 + 2 * 3) + 6 + gathers
    return pl.pallas_call(
        functools.partial(kernel, sizes, z_window, pairs),
        out_shape=[pltpu.VMEM(source.shape, jnp.float32)] * 2,
        in_specs=[pl.BlockSpec(memory_space=pl.ANY)] * 2,
        out_specs=[pl.BlockSpec(memory_space=pltpu.VMEM)] * 2,
        scratch_shapes=vmem(source.shape, 2) + vmem(inside, 1) + vmem(fine, 13)
        + vmem(mid, 10) + vmem(lifted, 1) + vmem(low, 8) + vmem(lifted_low, 1) + [
            pltpu.SemaphoreType.DMA((2,)),
            pltpu.SemaphoreType.DMA((copies,)),
            pltpu.SemaphoreType.DMA((copies,)),
        ],
        compiler_params=pltpu.CompilerParams(
            collective_id=0, has_side_effects=True, vmem_limit_bytes=56 * 1024 * 1024
        ),
    )(source, conduct)


def solution(mesh):
    spec = P("gz", "gy", None)
    sizes = (mesh.shape["gz"], mesh.shape["gy"])
    return jax.shard_map(
        functools.partial(local, sizes),
        mesh=mesh,
        in_specs=(spec, spec),
        out_specs=(spec, spec),
        check_vma=False,
    )
```

```python
import functools
import math

import jax
import jax.numpy as jnp
from jax import lax
from jax.experimental import pallas as pl
from jax.experimental.pallas import tpu as pltpu
from jax.sharding import PartitionSpec as P

DEGREE = 3
COARSE_DEGREE = 4

cheb_low = 0.3
cheb_high = 1.9
heat_step = 4.0

HALO = 4
PAD = 8
EDGE = 16
MID_REACH = 15
MESH = pl.DeviceIdType.MESH
LANES = 128
TILE = 8


def coefficients(steps):
    theta = (cheb_high + cheb_low) / 2.0
    delta = (cheb_high - cheb_low) / 2.0
    sigma = theta / delta
    rho = 1.0 / sigma
    pairs = [(0.0, 1.0 / theta)]
    for _ in range(steps - 1):
        rho_next = 1.0 / (2.0 * sigma - rho)
        pairs.append((rho_next * rho, 2.0 * rho_next / delta))
        rho = rho_next
    return pairs


def window(devices, reach):
    count = min(2 * reach + 1, devices)
    ahead = count // 2
    return [s if s <= ahead else s - count for s in range(count)]


def parts_of(value, count):
    parts = []
    for _ in range(count):
        parts.append(value.astype(jnp.bfloat16))
        value = value - parts[-1].astype(jnp.float32)
    return parts


def pick_columns(value, columns, count):
    total = None
    for part in reversed(parts_of(value, count)):
        term = jnp.dot(part, columns, preferred_element_type=jnp.float32)
        total = term if total is None else total + term
    return total


def unrolled(count, most):
    return max(u for u in range(1, most + 1) if count % u == 0)


def loop(count, body, most=16):
    def step(i, carry):
        body(i)
        return carry

    lax.fori_loop(0, count, step, 0, unroll=unrolled(count, most))


def rows_at(ref, p, c, row):
    return ref[p, c, pl.ds(row, TILE)]


def beside_of(w, p, row):
    planes, chunks = w.shape[0], w.shape[1]
    after, before = lax.rem(p + 1, planes), lax.rem(p + planes - 1, planes)
    here = [rows_at(w, p, c, row) for c in range(chunks)]
    lane = lax.broadcasted_iota(jnp.int32, here[0].shape, 1)
    first = jnp.where(lane == 0, 0.0, pltpu.roll(here[-1], 1, 1))
    last = jnp.where(lane == LANES - 1, 0.0, pltpu.roll(here[0], LANES - 1, 1))
    around = [first] + here + [last]
    beside = []
    for c in range(chunks):
        total = rows_at(w, after, c, row) + rows_at(w, before, c, row)
        total = total + (rows_at(w, p, c, row - 1) + rows_at(w, p, c, row + 1))
        beside.append(total + (around[c] + around[c + 2]))
    return here, beside


class Level:
    def __init__(self, k, m, g, inverse, d, wa, wb, rows, wraps):
        self.k, self.m, self.g, self.inverse, self.d = k, m, g, inverse, d
        self.w = (wa, wb)
        self.rows, self.wraps = rows, wraps

    def run(self, planes, body):
        first, count = planes

        def at(i):
            body(lax.rem(i + first, self.k.shape[0]))

        loop(count, at)

    def put(self, ref, p, c, row, value):
        ref[p, c, pl.ds(row, TILE)] = value
        if self.wraps:
            if row == self.rows[0]:
                ref[p, c, pl.ds(self.rows[-1] + TILE, 1)] = value[:1]
            if row == self.rows[-1]:
                ref[p, c, pl.ds(self.rows[0] - 1, 1)] = value[TILE - 1 :]

    def wrap(self, ref):
        def body(p):
            for c in range(ref.shape[1]):
                end = self.rows[-1] + TILE
                ref[p, c, pl.ds(end, 1)] = ref[p, c, pl.ds(self.rows[0], 1)]
                ref[p, c, pl.ds(self.rows[0] - 1, 1)] = ref[p, c, pl.ds(end - 1, 1)]

        loop(ref.shape[0], body)

    def second(self, u, new, planes, steps):
        start = coefficients(steps)[0][1]
        keep, gain = coefficients(steps)[1]
        mine, theirs = keep * start + gain * (1.0 - start), gain * start

        def body(p):
            for row in self.rows:
                here, beside = beside_of(u, p, row)
                for c in range(len(here)):
                    change = mine * here[c] + theirs * (rows_at(self.m, p, c, row) * beside[c])
                    self.d[p, c, pl.ds(row, TILE)] = change
                    self.put(new, p, c, row, start * here[c] + change)

        self.run(planes, body)

    def step(self, u, old, new, planes, pair, save=True, plus=None):
        keep, gain = pair

        def body(p):
            for row in self.rows:
                here, beside = beside_of(old, p, row)
                for c in range(len(here)):
                    pull = rows_at(self.m, p, c, row) * beside[c] + rows_at(u, p, c, row)
                    change = gain * (pull - here[c])
                    if keep:
                        change = keep * rows_at(self.d, p, c, row) + change
                    if save:
                        self.d[p, c, pl.ds(row, TILE)] = change
                    value = here[c] + change
                    if plus is not None:
                        value = value + rows_at(plus, p, c, row)
                    self.put(new, p, c, row, value)

        self.run(planes, body)

    def residual(self, u, w, out, planes, rows):
        def body(p):
            for row in rows:
                here, beside = beside_of(w, p, row)
                for c in range(len(here)):
                    pull = (rows_at(u, p, c, row) - here[c]) * rows_at(self.g, p, c, row)
                    out[p, c, pl.ds(row, TILE)] = pull + beside[c]

        self.run(planes, body)


def coarsen(fine, coarse, planes, rows, factor, m=None):
    def body(p):
        for c in range(coarse.shape[1]):
            for row in range(0, rows, TILE):
                total = None
                for half in range(2):
                    for chunk in (2 * c, 2 * c + 1):
                        for odd in range(2):
                            at = pl.ds(PAD + 2 * row + odd, TILE, stride=2)
                            term = fine[2 * p + half, chunk, at]
                            total = term if total is None else total + term
                total = total * factor
                if m is not None:
                    total = total * rows_at(m, p, c, PAD + row)
                coarse[p, c, pl.ds(PAD + row, TILE)] = total

    loop(planes, body)


def kernel(sizes, z_window, pairs, source, conduct, adjoint, residual,
           raw_f, raw_k, f0, k0, m0, g0, inv0, u0a, u0b, wa0, wb0, d0, ha, hb, ws, t0,
           k1, m1, g1, inv1, u1a, u1b, wa1, wb1, d1, t1, e0,
           k2, m2, g2, inv2, u2, wa2, wb2, d2, e1,
           tally, load_sem, send_sem, recv_sem):
    gz, gy = sizes
    own_z, own_y, nx = source.shape
    mz, my = own_z // 2, own_y // 2
    zs = k0.shape[0]
    mid_planes, low_planes = k1.shape[0], k2.shape[0]
    mid_rows, low_rows = k1.shape[2] - 2 * PAD, k2.shape[2] - 2 * PAD
    me_z, me_y = lax.axis_index("gz"), lax.axis_index("gy")
    core = lax.rem(me_y, 2)
    mate = 1 - 2 * core
    slots = 2 * len(pairs)

    def at(oz, oy):
        return (lax.rem(me_z + oz + gz, gz), lax.rem(me_y + oy + gy, gy))

    load_k = pltpu.make_async_copy(conduct, raw_k, load_sem.at[0])
    load_f = pltpu.make_async_copy(source, raw_f, load_sem.at[1])
    load_k.start()
    load_f.start()

    barrier = pltpu.get_barrier_semaphore()
    near = [-1, 0, 1]
    greet = {(oz % gz, oy % gy) for oz in near for oy in near}
    for s in z_window:
        greet |= {(s % gz, 0), (-s % gz, 0)}
    for s in pairs:
        greet |= {(0, 2 * s % gy), (0, -2 * s % gy)}
    greet = sorted(greet - {(0, 0)})
    for oz, oy in greet:
        pl.semaphore_signal(barrier, inc=1, device_id=at(oz, oy), device_id_type=MESH)

    share = nx // LANES

    def deal(r, c, value):
        pick = r == share * (c & (LANES - 1)) + c // LANES
        return jnp.where(pick, value, 0.0).astype(jnp.bfloat16)

    rows = lax.broadcasted_iota(jnp.int32, (nx, nx), 0)
    columns = lax.broadcasted_iota(jnp.int32, (nx, nx), 1)

    def enter(raw, out, row, value):
        flat = pick_columns(raw[...].reshape(own_z * own_y, nx), deal(rows, columns, value), 3)
        for p in range(own_z):
            for c in range(share):
                piece = flat[p * own_y : (p + 1) * own_y, c * LANES : (c + 1) * LANES]
                out[p, c, pl.ds(row, own_y)] = piece

    own_tiles = tuple(range(PAD, PAD + own_y, TILE))
    fine_tiles = tuple(range(PAD - HALO, PAD + own_y + HALO, TILE))
    fine = Level(k0, m0, g0, inv0, d0, wa0, wb0, fine_tiles, False)
    mid = Level(k1, m1, g1, inv1, d1, wa1, wb1, tuple(range(PAD, PAD + mid_rows, TILE)), True)
    low = Level(k2, m2, g2, inv2, d2, wa2, wb2, tuple(range(PAD, PAD + low_rows, TILE)), True)

    def around(margin):
        return (zs - margin, own_z + 2 * margin)

    def weigh(level, p, row, whole=True):
        for c in range(level.k.shape[1]):
            inverse = 1.0 / rows_at(level.k, p, c, row)
            g = 6.0 + inverse
            level.m[p, c, pl.ds(row, TILE)] = 1.0 / g
            if whole:
                level.g[p, c, pl.ds(row, TILE)] = g
                level.inverse[p, c, pl.ds(row, TILE)] = inverse

    load_k.wait()
    enter(raw_k, k0, PAD, heat_step)

    def own_weights(p):
        for row in own_tiles:
            weigh(fine, p, row)

    loop(own_z, own_weights)
    load_f.wait()
    enter(raw_f, f0, 0, 1.0)

    def own_start(p):
        for c in range(share):
            for row in own_tiles:
                value = rows_at(m0, p, c, row) * rows_at(f0, p, c, row - PAD)
                u0a[p, c, pl.ds(row, TILE)] = value

    loop(own_z, own_start)
    coarsen(k0, k1, mz, my, 0.125 / 4.0)

    def own_mid_weights(p):
        for row in range(PAD, PAD + my, TILE):
            weigh(mid, p, row)

    loop(mz, own_mid_weights)

    pl.semaphore_wait(barrier, len(greet))

    counts = {"send": 0, "recv": 0}
    unsent = []

    def take(kind):
        counts[kind] += 1
        sems = send_sem if kind == "send" else recv_sem
        return sems.at[counts[kind] - 1]

    def copy_of(from_ref, to_ref, sent, got, device):
        return pltpu.make_async_remote_copy(
            src_ref=from_ref, dst_ref=to_ref, send_sem=sent, recv_sem=got,
            device_id=device, device_id_type=MESH)

    shared, amounts = [], []

    def send(from_ref, to_ref, device):
        sent, got = shared[-1] if shared else (take("send"), take("recv"))
        copy = copy_of(from_ref, to_ref, sent, got, device)
        copy.start()
        if shared:
            amounts.append(math.prod(from_ref.shape) // LANES)
        else:
            unsent.append(copy)
        return copy

    def together(sends):
        pair = (take("send"), take("recv"))
        shared.append(pair)
        amounts.clear()
        sends()
        shared.pop()
        all_rows = tally.at[pl.ds(0, sum(amounts))]
        whole = copy_of(all_rows, all_rows, *pair, at(1, 0))
        unsent.append(whole)
        return [whole]

    odd = lax.rem(me_z, 2)
    sides = [2 * odd - 1, 1 - 2 * odd]

    def face(own, held, side, skip, depth, row_side, depth_y, device):
        up = side > 0
        count = depth - skip
        start = jnp.where(up, own_z - depth, skip)
        land = jnp.where(up, zs - depth, own_z + skip)
        if row_side == 0:
            row, to_row, height = PAD, PAD, own_y
        elif row_side > 0:
            row, to_row, height = PAD + own_y - depth_y, PAD - depth_y, depth_y
        else:
            row, to_row, height = PAD, PAD + own_y, depth_y
        return send(own.at[pl.ds(start, count), :, pl.ds(row, height)],
                    held.at[pl.ds(land, count), :, pl.ds(to_row, height)], device)

    def flank(own, held, row_side, skip, depth_y):
        planes, height = pl.ds(0, own_z), depth_y - skip
        if row_side > 0:
            row, to_row = PAD + own_y - depth_y, PAD - depth_y
        else:
            row, to_row = PAD + skip, PAD + own_y + skip
        return send(own.at[planes, :, pl.ds(row, height)],
                    held.at[planes, :, pl.ds(to_row, height)], at(0, row_side))

    def surround(jobs):
        return together(lambda: send_around(jobs))

    def send_around(jobs):
        copies = []
        for number, side in enumerate(sides):
            for ref, skip, depth, depth_y, corners in jobs:
                copies.append(face(ref, ref, side, skip, depth, 0, 0, at(side, 0)))
            for ref, skip, depth, depth_y, corners in jobs:
                for row_side in (1, -1):
                    for n, corner in enumerate(corners):
                        copies.append(face(ref, ref, side, n, n + 1, row_side, corner,
                                           at(side, row_side)))
            if number == 0:
                for ref, skip, depth, depth_y, corners in jobs:
                    for row_side in (1, -1):
                        copies.append(flank(ref, ref, row_side, skip, depth_y))
        return copies

    def beyond(ref):
        copies = [face(ref, ref, sides[1], 2, HALO, 0, 0, at(sides[1], 0))]
        for side in sides:
            for row_side in (1, -1):
                copies.append(face(ref, ref, side, 2, HALO - 1, row_side, 1, at(side, row_side)))
        return copies

    def relay(ref):
        up = sides[1] > 0
        start = jnp.where(up, own_z, zs - 2)
        land = jnp.where(up, zs - HALO, own_z + 2)
        own_rows = pl.ds(PAD, own_y)
        return [send(ref.at[pl.ds(start, 2), :, own_rows], ref.at[pl.ds(land, 2), :, own_rows],
                     at(2 * sides[1], 0))]

    def await_all(copies):
        for copy in copies:
            copy.wait_recv()

    far_first = sorted(range(len(z_window)), key=lambda s: -abs(z_window[s]))[:-1]

    class Gather:
        def __init__(self, held):
            self.held = held
            self.z = {}
            for s in far_first:
                self.z[s] = send(self.block(0, 0), self.block(s, 0), at(-z_window[s], 0))
            self.y = {n: (take("send"), take("recv")) for n in range(1, len(pairs))}
            self.spread(0)

        def rows(self, slot):
            return pl.ds(pl.multiple_of(PAD + slot * my, TILE), my)

        def block(self, s, slot):
            return self.held.at[pl.ds(s * mz, mz), :, self.rows(slot)]

        def column(self, slot):
            return self.held.at[:, :, self.rows(slot)]

        def spread(self, s):
            for n in range(1, len(pairs)):
                slot = 2 * pairs[n] % slots
                sent, got = self.y[n]
                copy_of(self.block(s, 0), self.block(s, slot), sent, got,
                        at(0, -2 * pairs[n])).start()

        def mirror(self, n):
            slot = 2 * pairs[n] % slots
            to_slot = lax.rem(slot - mate + slots, slots)
            return send(self.column(slot), self.column(to_slot), at(0, mate))

        def forward(self):
            for s in far_first:
                self.z[s].wait_recv()
                self.spread(s)
            self.mate = [self.mirror(0)]

        def across(self):
            for n in range(1, len(pairs)):
                slot = 2 * pairs[n] % slots
                whole = copy_of(self.column(0), self.column(slot), *self.y[n],
                                at(0, -2 * pairs[n]))
                whole.wait_recv()
                unsent.append(whole)
                self.mate.append(self.mirror(n))

        def wait(self):
            await_all(self.mate)

    first = surround([(u0a, 0, 3, 3, (2, 1)), (k0, 0, 2, HALO, (3, 2))])
    gather_k = Gather(k1)
    more = together(lambda: beyond(k0))
    await_all(first)
    more += relay(k0)

    steps = coefficients(DEGREE)

    def weights(p):
        for row in fine_tiles:
            weigh(fine, p, row, False)

    def some_weights(start, count):
        loop(count, lambda i: weights(lax.rem(i + start, zs)))

    some_weights(0, own_z + 2)
    some_weights(zs - 2, 2)

    def down(u, held, u1, between=None):
        fine.second(u, wa0, around(2), DEGREE)
        if between:
            between()
        fine.step(u, wa0, wb0, around(1), steps[2], save=False)
        fine.residual(u, wb0, t0, (0, own_z), own_tiles)
        coarsen(t0, u1, mz, my, 0.125, m1)
        gather = Gather(u1)

        def hold(p, edges=True):
            for c in range(share):
                for row in own_tiles:
                    held[p, c, pl.ds(row, TILE)] = rows_at(wb0, p, c, row)
                if edges:
                    for row in (PAD - 1, PAD + own_y):
                        held[p, c, pl.ds(row, 1)] = wb0[p, c, pl.ds(row, 1)]

        loop(own_z, hold)
        for p in (own_z, zs - 1):
            hold(p, False)
        return gather

    def solve(u1):
        everywhere = (0, mid_planes)
        mid.wrap(u1)
        mid.second(u1, wa1, everywhere, DEGREE)
        mid.step(u1, wa1, wb1, everywhere, steps[2], save=False)
        mid.residual(u1, wb1, t1, everywhere, mid.rows)
        coarsen(t1, u2, low_planes, low_rows, 0.125, m2)
        low.wrap(u2)
        low_steps = coefficients(COARSE_DEGREE)
        deep = (0, low_planes)
        low.second(u2, wa2, deep, COARSE_DEGREE)
        low.step(u2, wa2, wb2, deep, low_steps[2])
        low.step(u2, wb2, wa2, deep, low_steps[3], save=False)
        margin = HALO // 2 + DEGREE
        pairs_first, pairs_count = -(-margin // 2), mz // 2 + 2 * -(-margin // 2)
        pairs_count = min(pairs_count, low_planes)

        def lift(i):
            p = lax.rem(i + low_planes - pairs_first, low_planes)
            for row in low.rows:
                value = rows_at(wa2, p, 0, row) * rows_at(inv2, p, 0, row)
                spot = PAD + 2 * (row - PAD)
                for o in range(2):
                    e1[p, 0, pl.ds(spot + o, TILE, stride=2)] = value

        loop(pairs_count, lift)

        def add(i):
            p = lax.rem(i + low_planes - pairs_first, low_planes)
            for half in range(2):
                q = 2 * p + half
                for c in range(k1.shape[1]):
                    for row in mid.rows:
                        value = rows_at(wb1, q, c, row)
                        value = value + rows_at(k1, q, c, row) * rows_at(e1, p, c // 2, row)
                        mid.put(wb1, q, c, row, value)

        loop(pairs_count, add)

        def near_own(reach):
            if mz + 2 * reach >= mid_planes:
                return everywhere
            return (mid_planes - reach, mz + 2 * reach)

        reach = HALO // 2
        mid.step(u1, wb1, wa1, near_own(reach + 2), steps[0])
        mid.step(u1, wa1, wb1, near_own(reach + 1), steps[1])
        mid.step(u1, wb1, wa1, near_own(reach), steps[2], save=False)

        def lift_fine(i):
            q = lax.rem(i + mid_planes - reach, mid_planes)
            for c in range(k1.shape[1]):
                for row in range(-TILE, my + TILE, TILE):
                    here = PAD + row % mid_rows
                    value = rows_at(wa1, q, c, here) * rows_at(inv1, q, c, here)
                    for o in range(2):
                        e0[i, c, pl.ds(EDGE + 2 * row + o, TILE, stride=2)] = value

        loop(mz + 2 * reach, lift_fine)

    def up(u, held, out, plus=None):
        reach = HALO // 2

        def body(i):
            for half in range(2):
                p = lax.rem(2 * i + half + zs - HALO, zs)
                for c in range(share):
                    for row in fine_tiles:
                        add = rows_at(e0, i, c // 2, EDGE + row - PAD)
                        value = rows_at(held, p, c, row) + rows_at(k0, p, c, row) * add
                        wa0[p, c, pl.ds(row, TILE)] = value

        loop(mz + 2 * reach, body)
        fine.step(u, wa0, wb0, around(3), steps[0])
        fine.step(u, wb0, wa0, around(2), steps[1])
        fine.step(u, wa0, out, around(1), steps[2], save=False, plus=plus)

    def remain(p, row, w):
        here, beside = beside_of(w, p, row)
        values = []
        for c in range(share):
            pull = rows_at(f0, p, c, row - PAD) - rows_at(g0, p, c, row) * here[c]
            values.append(pull + beside[c])
        return here, values

    gather = down(u0a, ha, u1a, gather_k.forward)
    gather_k.across()
    held = surround([(ha, 1, HALO, HALO, (3, 2, 1))])
    gather.forward()
    gather_k.wait()

    def mid_weights(p):
        for row in mid.rows:
            weigh(mid, p, row)

    loop(mid_planes, mid_weights)
    coarsen(k1, k2, low_planes, low_rows, 0.125 / 4.0)

    def low_weights(p):
        for row in low.rows:
            weigh(low, p, row)

    loop(low_planes, low_weights)
    gather.across()
    gather.wait()
    solve(u1a)
    await_all(more)
    some_weights(own_z + 2, 1)
    some_weights(zs - 3, 1)
    await_all(held)
    up(u0a, ha, ws)

    def again(p):
        for row in own_tiles:
            _, values = remain(p, row, ws)
            for c in range(share):
                u0b[p, c, pl.ds(row, TILE)] = rows_at(m0, p, c, row) * values[c]

    loop(own_z, again)
    second = surround([(u0b, 0, 3, 3, (2, 1))])
    await_all(second)
    gather = down(u0b, hb, u1b)
    held = surround([(hb, 1, HALO, HALO, (3, 2, 1))])
    gather.forward()
    gather.across()
    gather.wait()
    solve(u1b)
    await_all(held)
    up(u0b, hb, wb0, plus=ws)

    back = deal(columns, rows, 1.0)

    def leave(pieces, out):
        flat = jnp.concatenate(pieces, axis=1)
        out[...] = pick_columns(flat, back, 2).reshape(own_z, own_y, nx)

    def finish(p):
        for row in own_tiles:
            _, values = remain(p, row, wb0)
            for c in range(share):
                t0[p, c, pl.ds(row, TILE)] = values[c]

    loop(own_z, finish)

    def pieces_of(ref, weight=None):
        pieces = []
        for c in range(share):
            parts = []
            for p in range(own_z):
                value = ref[p, c, pl.ds(PAD, own_y)]
                if weight is not None:
                    value = value * weight[p, c, pl.ds(PAD, own_y)]
                parts.append(value)
            pieces.append(jnp.concatenate(parts, axis=0))
        return pieces

    leave(pieces_of(wb0, inv0), adjoint)
    leave(pieces_of(t0), residual)
    for copy in unsent:
        copy.wait_send()
    assert counts["send"] <= send_sem.shape[0] and counts["recv"] <= recv_sem.shape[0], counts


def local(sizes, source, conduct):
    own_z, own_y, nx = source.shape
    z_window = window(sizes[0], -(-MID_REACH // (own_z // 2)))
    pairs = window(sizes[1] // 2, -(-MID_REACH // own_y))
    chunks = nx // LANES
    mz, my = own_z // 2, own_y // 2
    mid_planes, mid_rows = len(z_window) * mz, 2 * len(pairs) * my
    fine = (own_z + 2 * HALO, chunks, own_y + 2 * PAD, LANES)
    mid = (mid_planes, chunks // 2, mid_rows + 2 * PAD, LANES)
    low = (mid_planes // 2, chunks // 4, mid_rows // 2 + 2 * PAD, LANES)
    lifted = (mz + HALO, chunks // 2, own_y + 2 * EDGE, LANES)
    lifted_low = (mid_planes // 2, chunks // 4, mid_rows + 2 * PAD, LANES)
    inside = (own_z, chunks, own_y, LANES)
    vmem = lambda shape, count: [pltpu.VMEM(shape, jnp.float32)] * count
    gathers = 3 * (len(z_window) - 1 + 2 * len(pairs) - 1)
    copies = 6 + gathers
    return pl.pallas_call(
        functools.partial(kernel, sizes, z_window, pairs),
        out_shape=[pltpu.VMEM(source.shape, jnp.float32)] * 2,
        in_specs=[pl.BlockSpec(memory_space=pl.ANY)] * 2,
        out_specs=[pl.BlockSpec(memory_space=pltpu.VMEM)] * 2,
        scratch_shapes=vmem(source.shape, 2) + vmem(inside, 1) + vmem(fine, 13)
        + vmem(mid, 10) + vmem(lifted, 1) + vmem(low, 8) + vmem(lifted_low, 1) + [
            pltpu.VMEM((2 * fine[0] * chunks * own_y, LANES), jnp.float32),
            pltpu.SemaphoreType.DMA((2,)),
            pltpu.SemaphoreType.DMA((copies,)),
            pltpu.SemaphoreType.DMA((copies,)),
        ],
        compiler_params=pltpu.CompilerParams(
            collective_id=0, has_side_effects=True, vmem_limit_bytes=56 * 1024 * 1024
        ),
    )(source, conduct)


def solution(mesh):
    spec = P("gz", "gy", None)
    sizes = (mesh.shape["gz"], mesh.shape["gy"])
    return jax.shard_map(
        functools.partial(local, sizes),
        mesh=mesh,
        in_specs=(spec, spec),
        out_specs=(spec, spec),
        check_vma=False,
    )
```
